32 devices in a mesh: rows: 4 (over z), cols: 8 (over y, x, core).
Axes of the slice: x: 2, y: 2, z: 4, core: 2. Of those that a mesh axis runs over, the one named last changes fastest.
Arguments:
- spectra: float32 [224, 16, 1024], P(None, 'rows', 'cols'), may hold values from -23 to 23
- library: float32 [224, 240], replicated, may hold values from -0.375 to 0.375
Outputs:
- abundance: float32 [240, 16, 1024], P(None, 'rows', 'cols')
- residual_norms: float32 [4, 2], replicated
The draws below stay inside these ranges and needn't reach their ends.
All inputs are finite; a program needn't handle non-finite values.
Results may differ from the reference program's by a relative error of at most 0.0001.
Values sent between devices are 32-bit elements; how exact they have to be, the bound alone decides.
A program may use at most 64 MiB of HBM per device.

```python
import jax
import jax.numpy as jnp
from jax import lax

BANDS = 224
ENDM = 240
ITERS = 4
SWEEPS = 2
IMG_ROWS = 16
IMG_COLS = 1024


def draw_spectra(key, part):
    key_base = jax.random.fold_in(key, 11)
    key_rough = jax.random.fold_in(key, 12)
    row_pos = jnp.arange(IMG_ROWS, dtype=jnp.float32) / max(IMG_ROWS - 1, 1)
    col_pos = jnp.arange(IMG_COLS, dtype=jnp.float32) / max(IMG_COLS - 1, 1)
    scale = jnp.exp(jnp.log(3.0) * 0.5 * (row_pos[:, None] + col_pos[None, :]))
    rough = jax.random.uniform(key_rough, (1, IMG_ROWS, IMG_COLS), jnp.float32, 0.5, 1.5)
    base = jnp.clip(jax.random.normal(key_base, (BANDS, IMG_ROWS, IMG_COLS), jnp.float32), -5.0, 5.0)
    return (base * scale[None, :, :] * rough).astype(jnp.float32)


def normal_values(rng, shape, width, reach, kind=jnp.bfloat16):
    array = width * jax.random.normal(rng, shape, jnp.float32)
    return jnp.clip(array, min=-reach, max=reach).astype(kind)


def setup_inputs(seed: int = 0) -> dict:
    seeds = jax.random.split(jax.random.key(seed), 3)
    spectra = draw_spectra(jax.random.fold_in(seeds[2], 71), 0)
    library = normal_values(seeds[1], (BANDS, ENDM), BANDS ** -0.5, 0.375, jnp.float32)
    return {"spectra": spectra, "library": library}


MU = 0.5
LAMBDA = 0.02
LAMBDA_TV = 0.05

def soft(value, thresh):
    return value - jnp.clip(value, -thresh, thresh)

def apply_matrix(matrix, field):
    flat = field.reshape(field.shape[0], -1)
    out = jnp.dot(matrix.astype(jnp.float32), flat.astype(jnp.float32), precision=lax.Precision.HIGHEST, preferred_element_type=jnp.float32)
    return out.reshape(matrix.shape[0], field.shape[1], field.shape[2])

def inverse_of(library):
    count = library.shape[1]
    ident = jnp.eye(count, dtype=jnp.float32)
    gram = jnp.dot(library.T, library, precision=lax.Precision.HIGHEST) + 3.0 * ident
    factor = jnp.linalg.cholesky(gram)
    return jax.scipy.linalg.cho_solve((factor, True), ident)

def reference(spectra, library):
    inverse = inverse_of(library)
    zeros = jnp.zeros((ENDM, IMG_ROWS, IMG_COLS), jnp.float32)
    v1, v2, v3, v4h, v4v, v5 = (spectra, zeros, zeros, zeros, zeros, zeros)
    d1 = jnp.zeros_like(spectra)
    d2, d3, d4h, d4v, d5 = (zeros, zeros, zeros, zeros, zeros)
    numel = float(ENDM * IMG_ROWS * IMG_COLS)
    table = []
    for step in range(ITERS):
        mixed = apply_matrix(library.T, v1 + d1) + (v2 + d2) + (v3 + d3) + (v5 + d5)
        abundance = apply_matrix(inverse, mixed)
        image = apply_matrix(library, abundance)
        new1 = (spectra + MU * (image - d1)) / (1.0 + MU)
        new2 = soft(abundance - d2, LAMBDA / MU)
        new5 = jnp.maximum(abundance - d5, 0.0)
        horiz = v4h + d4h
        vert = v4v + d4v
        back = jnp.roll(horiz, 1, 2) - horiz + (jnp.roll(vert, 1, 1) - vert)
        rhs = abundance - d3 + back
        smooth = v3
        for sweep in range(SWEEPS):
            near = jnp.roll(smooth, 1, 1) + jnp.roll(smooth, -1, 1) + jnp.roll(smooth, 1, 2) + jnp.roll(smooth, -1, 2)
            smooth = (rhs + near) / 5.0
        new3 = smooth
        grad_h = jnp.roll(new3, -1, 2) - new3
        grad_v = jnp.roll(new3, -1, 1) - new3
        new4h = soft(grad_h - d4h, LAMBDA_TV / MU)
        new4v = soft(grad_v - d4v, LAMBDA_TV / MU)
        r1 = image - new1
        r2 = abundance - new2
        r3 = abundance - new3
        r4h = grad_h - new4h
        r4v = grad_v - new4v
        r5 = abundance - new5
        primal = jnp.sum(r1 * r1) + jnp.sum(r2 * r2) + jnp.sum(r3 * r3) + jnp.sum(r4h * r4h) + jnp.sum(r4v * r4v) + jnp.sum(r5 * r5)
        c1 = new1 - v1
        c2 = new2 - v2
        c3 = new3 - v3
        c4h = new4h - v4h
        c4v = new4v - v4v
        c5 = new5 - v5
        dual = MU * MU * (jnp.sum(c1 * c1) + jnp.sum(c2 * c2) + jnp.sum(c3 * c3) + jnp.sum(c4h * c4h) + jnp.sum(c4v * c4v) + jnp.sum(c5 * c5))
        table.append(jnp.stack([jnp.sqrt(primal / numel), jnp.sqrt(dual / numel)]))
        d1, d2, d3, d4h, d4v, d5 = (d1 - r1, d2 - r2, d3 - r3, d4h - r4h, d4v - r4v, d5 - r5)
        v1, v2, v3, v4h, v4v, v5 = (new1, new2, new3, new4h, new4v, new5)
    return (abundance, jnp.stack(table).astype(jnp.float32))
```

```python
import functools

import jax
import jax.numpy as jnp
from jax import lax
from jax.experimental import pallas as pl
from jax.experimental.pallas import tpu as pltpu
from jax.sharding import PartitionSpec as P

ITERS = 4
MU = 0.5
LAMBDA = 0.02
LAMBDA_TV = 0.05
SHIFT = 3.0
NEWTON = 8
CH = 16
F32 = jnp.float32
BF16 = jnp.bfloat16


def split(value):
    high = value.astype(BF16)
    return high, (value - high.astype(F32)).astype(BF16)


def dot(lhs, rhs):
    return jnp.dot(lhs, rhs, preferred_element_type=F32)


def dot_full(lhs, rhs):
    return jnp.dot(lhs, rhs, precision=lax.Precision.HIGHEST, preferred_element_type=F32)


def kernel(
    dims, spec_ref, lib_ref, libt_ref, out_ref, norm_ref,
    inv3, lib3, libt3, rhs3, newton_x, newton_r, gram,
    abun, image, mixed, rhs, v1, d1, v2, d2, v5, d5, d3, v4h, d4h, v4v, d4v, d4g, d4c,
    w1, w3, rowbuf, colbuf, colsend, send_sem, recv_sem,
):
    bands, endm, rows, cols, n_rows, n_cols, pad = dims
    me_r, me_c = lax.axis_index("rows"), lax.axis_index("cols")
    up = (lax.rem(me_r + n_rows - 1, n_rows), me_c)
    down = (lax.rem(me_r + 1, n_rows), me_c)
    left = (me_r, lax.rem(me_c + n_cols - 1, n_cols))
    right = (me_r, lax.rem(me_c + 1, n_cols))
    mesh_type = pl.DeviceIdType.MESH
    barrier = pltpu.get_barrier_semaphore()
    for target in (up, down, left, right):
        pl.semaphore_signal(barrier, inc=1, device_id=target, device_id_type=mesh_type)

    lane = lax.broadcasted_iota(jnp.int32, (8, cols), 1)

    def lanes(r):
        return slice(r * cols, (r + 1) * cols)

    def stack_lhs(ref, value):
        high, low = split(value)
        ref[:, 0:pad] = high
        ref[:, pad : 2 * pad] = high
        ref[:, 2 * pad : 3 * pad] = low

    def put_rhs(at, r, value):
        high, low = split(value)
        rhs3[pl.ds(at, CH), lanes(r)] = high
        rhs3[pl.ds(at + pad, CH), lanes(r)] = low
        rhs3[pl.ds(at + 2 * pad, CH), lanes(r)] = high

    def fold(value):
        total = value[0:8]
        for i in range(8, CH, 8):
            total = total + value[i : i + 8]
        return total

    def chunks(count, body, init):
        def step(i, carry):
            return body(i, pl.multiple_of(i * CH, CH), carry)

        return lax.fori_loop(0, count // CH, step, init)

    zero = jnp.zeros((8, cols), F32)

    def load_spectra(i, at, carry):
        for r in range(rows):
            value = spec_ref[pl.ds(at, CH), r, :]
            v1[pl.ds(at, CH), lanes(r)] = value
            d1[pl.ds(at, CH), lanes(r)] = jnp.zeros((CH, cols), F32)
            put_rhs(at, r, value)
        return carry

    for base in (0, pad, 2 * pad):
        rhs3[base + bands : base + pad, :] = jnp.zeros((pad - bands, rows * cols), BF16)
    chunks(bands, load_spectra, 0)

    stack_lhs(lib3, lib_ref[...])
    stack_lhs(libt3, libt_ref[...])
    mixed[...] = dot(libt3[...], rhs3[...])
    eye = (
        lax.broadcasted_iota(jnp.int32, (pad, pad), 0)
        == lax.broadcasted_iota(jnp.int32, (pad, pad), 1)
    ).astype(F32)
    gram[...] = dot_full(libt_ref[...], lib_ref[...]) + SHIFT * eye
    bound = jnp.max(jnp.sum(jnp.abs(gram[...]), axis=1, keepdims=True), axis=0, keepdims=True)
    scale = 2.0 / (SHIFT + bound)
    newton_x[...] = eye * scale
    newton_r[...] = eye - gram[...] * scale

    def newton(_, radius):
        square = radius * radius
        factor = 2.0 / (2.0 - square)
        r_val = newton_r[...]
        x_val = newton_x[...]
        r_hi, r_lo = split(r_val)
        x_hi, x_lo = split(x_val)
        r_next = dot(r_hi, r_hi) + dot(r_hi, r_lo) + dot(r_lo, r_hi)
        x_next = dot(x_hi, r_hi) + dot(x_hi, r_lo) + dot(x_lo, r_hi)
        newton_x[...] = factor * (x_val + x_next)
        newton_r[...] = (1.0 - factor) * eye + factor * r_next
        return square / (2.0 - square)

    lax.fori_loop(0, NEWTON, newton, (bound - SHIFT) / (bound + SHIFT))
    for _ in range(2):
        newton_r[...] = eye - dot_full(gram[...], newton_x[...])
        newton_x[...] = newton_x[...] + dot_full(newton_x[...], newton_r[...])
    stack_lhs(inv3, newton_x[...])

    def put_mixed(i, at, carry):
        for r in range(rows):
            put_rhs(at, r, mixed[pl.ds(at, CH), lanes(r)])
        return carry

    for base in (0, pad, 2 * pad):
        rhs3[base + endm : base + pad, :] = jnp.zeros((pad - endm, rows * cols), BF16)
    chunks(endm, put_mixed, 0)
    pl.semaphore_wait(barrier, 4)

    def pack(i, values, firsts, lasts):
        for half in range(CH // 8):
            for r in range(rows):
                spot = (i * (CH // 8) + half) * rows + r
                part = values[r][8 * half : 8 * half + 8]
                hit = lane == spot
                firsts = jnp.where(hit, pltpu.roll(part, spot, 1), firsts)
                lasts = jnp.where(hit, pltpu.roll(part, lax.rem(spot + 1, cols), 1), lasts)
        return firsts, lasts

    def unpack(i, r, packed, spot_to):
        parts = []
        for half in range(CH // 8):
            spot = (i * (CH // 8) + half) * rows + r
            parts.append(pltpu.roll(packed, lax.rem(spot_to - spot + cols, cols), 1))
        return jnp.concatenate(parts, axis=0)

    wide_lane = lax.broadcasted_iota(jnp.int32, (CH, cols), 1)

    def from_left(i, r, value, packed):
        return jnp.where(wide_lane == 0, unpack(i, r, packed, 0), pltpu.roll(value, 1, 1))

    def from_right(i, r, value, packed):
        return jnp.where(
            wide_lane == cols - 1, unpack(i, r, packed, cols - 1), pltpu.roll(value, cols - 1, 1)
        )

    def copies(e, source, ends):
        table = []
        for side in ends:
            src, dst, target = (
                (source.at[:, lanes(rows - 1)], rowbuf.at[e, 0], down),
                (source.at[:, lanes(0)], rowbuf.at[e, 1], up),
                (colsend.at[e, 1], colbuf.at[e, 0], right),
                (colsend.at[e, 0], colbuf.at[e, 1], left),
            )[side]
            table.append(
                pltpu.make_async_remote_copy(
                    src_ref=src, dst_ref=dst, send_sem=send_sem.at[e, side],
                    recv_sem=recv_sem.at[e, side], device_id=target, device_id_type=mesh_type,
                )
            )
        return table

    pending = []

    def send(e, source, firsts, lasts, ends=(0, 1, 2, 3)):
        colsend[e, 0] = firsts
        colsend[e, 1] = lasts
        table = copies(e, source, ends)
        for copy in table:
            copy.start()
        pending.extend(table)
        return table

    def receive(table):
        for copy in table:
            copy.wait_recv()

    thresh = LAMBDA / MU
    thresh_tv = LAMBDA_TV / MU

    def gradients(k, in_flight, last):
        e = 2 * (k - 1) + 1
        receive(in_flight)
        source = w3.at[k - 1]
        first_time = k == 1
        pl_left = None if last else colbuf[e, 0]
        pl_right = colbuf[e, 1]
        if not last:
            grad = colsend[e, 0] - pl_left
            ghost = grad if first_time else grad - d4c[...]
            clipped = jnp.clip(ghost, -thresh_tv, thresh_tv)
            d4c[...] = -clipped
            ghost_h = ghost - 2.0 * clipped

        def body(i, at, carry):
            primal, dual, firsts, lasts = carry
            rs = pl.ds(at, CH)
            x = [source[rs, lanes(r)] for r in range(rows)]
            below = rowbuf[e, 1, rs, :]
            if not last:
                above = rowbuf[e, 0, rs, :]
                ghost_v = x[0] - above
                if not first_time:
                    ghost_v = ghost_v - d4g[rs, :]
                cut = jnp.clip(ghost_v, -thresh_tv, thresh_tv)
                d4g[rs, :] = -cut
                over = ghost_v - 2.0 * cut
            results = []
            for r in range(rows):
                nxt = x[r + 1] if r + 1 < rows else below
                x_right = from_right(i, r, x[r], pl_right)
                sums = []
                for grad_now, v_ref, d_ref in (
                    (x_right - x[r], v4h, d4h), (nxt - x[r], v4v, d4v),
                ):
                    u = grad_now if first_time else grad_now - d_ref[rs, lanes(r)]
                    cut = jnp.clip(u, -thresh_tv, thresh_tv)
                    new = u - cut
                    res = cut if first_time else d_ref[rs, lanes(r)] + cut
                    change = new if first_time else new - v_ref[rs, lanes(r)]
                    primal = primal + fold(res * res)
                    dual = dual + fold(change * change)
                    if not last:
                        d_ref[rs, lanes(r)] = -cut
                        v_ref[rs, lanes(r)] = new
                        sums.append(new - cut)
                if not last:
                    x_left = from_left(i, r, x[r], pl_left)
                    h_left = from_left(i, r, sums[0], ghost_h)
                    back = (h_left - sums[0]) + (over - sums[1])
                    over = sums[1]
                    total = abun[rs, lanes(r)] - d3[rs, lanes(r)] + back
                    rhs[rs, lanes(r)] = total
                    prv = x[r - 1] if r else above
                    new_w = (total + ((prv + nxt) + (x_left + x_right))) * 0.2
                    w1[k, rs, lanes(r)] = new_w
                    results.append(new_w)
            if not last:
                firsts, lasts = pack(i, results, firsts, lasts)
            return primal, dual, firsts, lasts

        return chunks(endm, body, (zero, zero, zero, zero))

    def first_sweep(i, at, carry):
        rs = pl.ds(at, CH)
        results = []
        for r in range(rows):
            value = abun[rs, lanes(r)] * 0.2
            w1[0, rs, lanes(r)] = value
            results.append(value)
        return pack(i, results, *carry)

    def data_terms(first_time, last):
        def body(i, at, carry):
            primal, dual = carry
            rs = pl.ds(at, CH)
            for r in range(rows):
                old = d1[rs, lanes(r)]
                u = image[rs, lanes(r)] - old
                new = (spec_ref[rs, r, :] + MU * u) / (1.0 + MU)
                d_new = new - u
                res = old - d_new
                change = new - v1[rs, lanes(r)]
                primal = primal + fold(res * res)
                dual = dual + fold(change * change)
                if not last:
                    d1[rs, lanes(r)] = d_new
                    v1[rs, lanes(r)] = new
                    put_rhs(at, r, new + d_new)
            return primal, dual

        return body

    def point_terms(first_time, last):
        def body(i, at, carry):
            primal, dual = carry
            rs = pl.ds(at, CH)
            for r in range(rows):
                a = abun[rs, lanes(r)]
                old2 = None if first_time else d2[rs, lanes(r)]
                u2 = a if first_time else a - old2
                cut = jnp.clip(u2, -thresh, thresh)
                new2 = u2 - cut
                res2 = cut if first_time else old2 + cut
                change2 = new2 if first_time else new2 - v2[rs, lanes(r)]
                old5 = None if first_time else d5[rs, lanes(r)]
                u5 = a if first_time else a - old5
                new5 = jnp.maximum(u5, 0.0)
                res5 = a - new5
                change5 = new5 if first_time else new5 - v5[rs, lanes(r)]
                primal = primal + fold(res2 * res2 + res5 * res5)
                dual = dual + fold(change2 * change2 + change5 * change5)
                if last:
                    out_ref[rs, r, :] = a
                else:
                    d2[rs, lanes(r)] = -cut
                    v2[rs, lanes(r)] = new2
                    v5[rs, lanes(r)] = new5
                    d5[rs, lanes(r)] = new5 - u5
                    mixed[rs, lanes(r)] = mixed[rs, lanes(r)] + ((new2 - cut) + jnp.abs(u5))
            return primal, dual

        return body

    def second_sweep(k, last):
        e = 2 * k
        source = w1.at[k]
        first_time = k == 0
        pl_left = colbuf[e, 0]
        pl_right = colbuf[e, 1]

        def body(i, at, carry):
            primal, dual, firsts, lasts = carry
            rs = pl.ds(at, CH)
            x = [source[rs, lanes(r)] for r in range(rows)]
            above = rowbuf[e, 0, rs, :]
            below = rowbuf[e, 1, rs, :]
            results = []
            for r in range(rows):
                nxt = x[r + 1] if r + 1 < rows else below
                prv = x[r - 1] if r else above
                near = (prv + nxt) + (
                    from_left(i, r, x[r], pl_left) + from_right(i, r, x[r], pl_right)
                )
                a = abun[rs, lanes(r)]
                total = a if first_time else rhs[rs, lanes(r)]
                new = (total + near) * 0.2
                w3[k, rs, lanes(r)] = new
                results.append(new)
                res = a - new
                change = new if first_time else new - w3[k - 1, rs, lanes(r)]
                primal = primal + fold(res * res)
                dual = dual + fold(change * change)
                if not last:
                    d_new = new - a if first_time else new - (a - d3[rs, lanes(r)])
                    d3[rs, lanes(r)] = d_new
                    put_rhs(at, r, mixed[rs, lanes(r)] + (new + d_new))
            firsts, lasts = pack(i, results, firsts, lasts)
            return primal, dual, firsts, lasts

        return chunks(endm, body, (zero, zero, zero, zero))

    table = None
    partial = [[zero, zero] for _ in range(ITERS)]

    def add(k, pair):
        partial[k][0] = partial[k][0] + pair[0]
        partial[k][1] = partial[k][1] + pair[1]

    for k in range(ITERS):
        last = k == ITERS - 1
        abun[...] = dot(inv3[...], rhs3[...])
        if k == 0:
            firsts, lasts = chunks(endm, first_sweep, (zero, zero))
        else:
            primal, dual, firsts, lasts = gradients(k, table, False)
            add(k - 1, (primal, dual))
        table = send(2 * k, w1.at[k], firsts, lasts)

        def put_abun(i, at, carry):
            for r in range(rows):
                put_rhs(at, r, abun[pl.ds(at, CH), lanes(r)])
            return carry

        chunks(endm, put_abun, 0)
        image[...] = dot(lib3[...], rhs3[...])
        add(k, chunks(bands, data_terms(k == 0, last), (zero, zero)))
        if not last:
            for base in (0, pad, 2 * pad):
                rhs3[base + bands : base + endm, :] = jnp.zeros((endm - bands, rows * cols), BF16)
            mixed[...] = dot(libt3[...], rhs3[...])
        add(k, chunks(endm, point_terms(k == 0, last), (zero, zero)))
        receive(table)
        primal, dual, firsts, lasts = second_sweep(k, last)
        add(k, (primal, dual))
        table = send(2 * k + 1, w3.at[k], firsts, lasts, (1, 3) if last else (0, 1, 2, 3))
    add(ITERS - 1, gradients(ITERS, table, True)[:2])
    for k in range(ITERS):
        norm_ref[2 * k] = partial[k][0]
        norm_ref[2 * k + 1] = partial[k][1] * (MU * MU)
    for copy in pending:
        copy.wait_send()


def local(spectra, library):
    bands, rows, cols = spectra.shape
    endm = library.shape[1]
    n_rows, n_cols = lax.axis_size("rows"), lax.axis_size("cols")
    pad = -(-max(bands, endm) // 256) * 256
    lib = jnp.pad(library, ((0, pad - bands), (0, pad - endm)))
    wide = rows * cols
    dims = (bands, endm, rows, cols, n_rows, n_cols, pad)
    field = pltpu.VMEM((endm, wide), F32)
    full = pltpu.VMEM((pad, wide), F32)
    band = pltpu.VMEM((bands, wide), F32)
    square = pltpu.VMEM((pad, pad), F32)
    stacked = pltpu.VMEM((pad, 3 * pad), BF16)
    exchanges = 2 * ITERS
    abundance, norms = pl.pallas_call(
        functools.partial(kernel, dims),
        out_shape=(
            jax.ShapeDtypeStruct((endm, rows, cols), F32),
            jax.ShapeDtypeStruct((2 * ITERS, 8, cols), F32),
        ),
        in_specs=[pl.BlockSpec(memory_space=pltpu.VMEM)] * 3,
        out_specs=(pl.BlockSpec(memory_space=pltpu.VMEM),) * 2,
        scratch_shapes=[
            stacked, stacked, stacked, pltpu.VMEM((3 * pad, wide), BF16),
            square, square, square,
            full, full, full, field, band, band, field, field, field, field, field,
            field, field, field, field, pltpu.VMEM((endm, cols), F32), pltpu.VMEM((8, cols), F32),
            pltpu.VMEM((ITERS, endm, wide), F32), pltpu.VMEM((ITERS, endm, wide), F32),
            pltpu.VMEM((exchanges, 2, endm, cols), F32),
            pltpu.VMEM((exchanges, 2, 8, cols), F32),
            pltpu.VMEM((exchanges, 2, 8, cols), F32),
            pltpu.SemaphoreType.DMA((exchanges, 4)),
            pltpu.SemaphoreType.DMA((exchanges, 4)),
        ],
        compiler_params=pltpu.CompilerParams(
            collective_id=0, has_side_effects=True, vmem_limit_bytes=56 * 1024 * 1024
        ),
    )(spectra, lib, lib.T)
    totals = lax.psum(jnp.sum(norms, axis=(1, 2)).reshape(ITERS, 2), ("rows", "cols"))
    numel = float(endm * rows * cols * n_rows * n_cols)
    return abundance, jnp.sqrt(totals / numel)


def solution(mesh):
    placed = (P(None, "rows", "cols"), P())
    return jax.shard_map(
        local, mesh=mesh, in_specs=placed, out_specs=(P(None, "rows", "cols"), P()), check_vma=False
    )
```

```python
import functools

import jax
import jax.numpy as jnp
from jax import lax
from jax.experimental import pallas as pl
from jax.experimental.pallas import tpu as pltpu
from jax.sharding import PartitionSpec as P

ITERS = 4
MU = 0.5
LAMBDA = 0.02
LAMBDA_TV = 0.05
SHIFT = 3.0
NEWTON = 8
CH = 16
F32 = jnp.float32
BF16 = jnp.bfloat16


def split(value):
    high = value.astype(BF16)
    return high, (value - high.astype(F32)).astype(BF16)


def dot(lhs, rhs):
    return jnp.dot(lhs, rhs, preferred_element_type=F32)


def dot_full(lhs, rhs):
    return jnp.dot(lhs, rhs, precision=lax.Precision.HIGHEST, preferred_element_type=F32)


def kernel(
    dims, spec_ref, lib_ref, libt_ref, out_ref, norm_ref,
    inv3, lib3, libt3, rhs3, newton_x, newton_r, gram,
    abun, image, mixed, rhs, v1, d1, v2, d2, v5, d5, d3, v4h, d4h, v4v, d4v, d4g, d4c,
    w1, w3, rowbuf, colbuf, colsend, send_sem, recv_sem,
    summing, row_slots, col_slots, sum_send, sum_recv,
):
    bands, endm, rows, cols, n_rows, n_cols, pad = dims
    me_r, me_c = lax.axis_index("rows"), lax.axis_index("cols")
    up = (lax.rem(me_r + n_rows - 1, n_rows), me_c)
    down = (lax.rem(me_r + 1, n_rows), me_c)
    left = (me_r, lax.rem(me_c + n_cols - 1, n_cols))
    right = (me_r, lax.rem(me_c + 1, n_cols))
    mesh_type = pl.DeviceIdType.MESH
    barrier = pltpu.get_barrier_semaphore()
    row_peers = [(lax.rem(me_r + step, n_rows), me_c) for step in range(1, n_rows)]
    col_peers = [(me_r, lax.rem(me_c + step, n_cols)) for step in range(1, n_cols)]
    for target in row_peers + col_peers:
        pl.semaphore_signal(barrier, inc=1, device_id=target, device_id_type=mesh_type)

    lane = lax.broadcasted_iota(jnp.int32, (8, cols), 1)

    def lanes(r):
        return slice(r * cols, (r + 1) * cols)

    def stack_lhs(ref, value):
        high, low = split(value)
        ref[:, 0:pad] = high
        ref[:, pad : 2 * pad] = high
        ref[:, 2 * pad : 3 * pad] = low

    def put_rhs(at, r, value):
        high, low = split(value)
        rhs3[pl.ds(at, CH), lanes(r)] = high
        rhs3[pl.ds(at + pad, CH), lanes(r)] = low
        rhs3[pl.ds(at + 2 * pad, CH), lanes(r)] = high

    def fold(value):
        total = value[0:8]
        for i in range(8, CH, 8):
            total = total + value[i : i + 8]
        return total

    def chunks(count, body, init):
        def step(i, carry):
            return body(i, pl.multiple_of(i * CH, CH), carry)

        return lax.fori_loop(0, count // CH, step, init)

    zero = jnp.zeros((8, cols), F32)

    def load_spectra(i, at, carry):
        for r in range(rows):
            value = spec_ref[pl.ds(at, CH), r, :]
            v1[pl.ds(at, CH), lanes(r)] = value
            d1[pl.ds(at, CH), lanes(r)] = jnp.zeros((CH, cols), F32)
            put_rhs(at, r, value)
        return carry

    for base in (0, pad, 2 * pad):
        rhs3[base + bands : base + pad, :] = jnp.zeros((pad - bands, rows * cols), BF16)
    chunks(bands, load_spectra, 0)

    stack_lhs(lib3, lib_ref[...])
    stack_lhs(libt3, libt_ref[...])
    mixed[...] = dot(libt3[...], rhs3[...])
    eye = (
        lax.broadcasted_iota(jnp.int32, (pad, pad), 0)
        == lax.broadcasted_iota(jnp.int32, (pad, pad), 1)
    ).astype(F32)
    gram[...] = dot_full(libt_ref[...], lib_ref[...]) + SHIFT * eye
    bound = jnp.max(jnp.sum(jnp.abs(gram[...]), axis=1, keepdims=True), axis=0, keepdims=True)
    scale = 2.0 / (SHIFT + bound)
    newton_x[...] = eye * scale
    newton_r[...] = eye - gram[...] * scale

    def newton(_, radius):
        square = radius * radius
        factor = 2.0 / (2.0 - square)
        r_val = newton_r[...]
        x_val = newton_x[...]
        r_hi, r_lo = split(r_val)
        x_hi, x_lo = split(x_val)
        r_next = dot(r_hi, r_hi) + dot(r_hi, r_lo) + dot(r_lo, r_hi)
        x_next = dot(x_hi, r_hi) + dot(x_hi, r_lo) + dot(x_lo, r_hi)
        newton_x[...] = factor * (x_val + x_next)
        newton_r[...] = (1.0 - factor) * eye + factor * r_next
        return square / (2.0 - square)

    lax.fori_loop(0, NEWTON, newton, (bound - SHIFT) / (bound + SHIFT))
    for _ in range(2):
        newton_r[...] = eye - dot_full(gram[...], newton_x[...])
        newton_x[...] = newton_x[...] + dot_full(newton_x[...], newton_r[...])
    stack_lhs(inv3, newton_x[...])

    def put_mixed(i, at, carry):
        for r in range(rows):
            put_rhs(at, r, mixed[pl.ds(at, CH), lanes(r)])
        return carry

    for base in (0, pad, 2 * pad):
        rhs3[base + endm : base + pad, :] = jnp.zeros((pad - endm, rows * cols), BF16)
    chunks(endm, put_mixed, 0)
    pl.semaphore_wait(barrier, n_rows + n_cols - 2)

    def pack(i, values, firsts, lasts):
        for half in range(CH // 8):
            for r in range(rows):
                spot = (i * (CH // 8) + half) * rows + r
                part = values[r][8 * half : 8 * half + 8]
                hit = lane == spot
                firsts = jnp.where(hit, pltpu.roll(part, spot, 1), firsts)
                lasts = jnp.where(hit, pltpu.roll(part, lax.rem(spot + 1, cols), 1), lasts)
        return firsts, lasts

    def unpack(i, r, packed, spot_to):
        parts = []
        for half in range(CH // 8):
            spot = (i * (CH // 8) + half) * rows + r
            parts.append(pltpu.roll(packed, lax.rem(spot_to - spot + cols, cols), 1))
        return jnp.concatenate(parts, axis=0)

    wide_lane = lax.broadcasted_iota(jnp.int32, (CH, cols), 1)

    def from_left(i, r, value, packed):
        return jnp.where(wide_lane == 0, unpack(i, r, packed, 0), pltpu.roll(value, 1, 1))

    def from_right(i, r, value, packed):
        return jnp.where(
            wide_lane == cols - 1, unpack(i, r, packed, cols - 1), pltpu.roll(value, cols - 1, 1)
        )

    def copies(e, source, ends):
        table = []
        for side in ends:
            src, dst, target = (
                (source.at[:, lanes(rows - 1)], rowbuf.at[e, 0], down),
                (source.at[:, lanes(0)], rowbuf.at[e, 1], up),
                (colsend.at[e, 1], colbuf.at[e, 0], right),
                (colsend.at[e, 0], colbuf.at[e, 1], left),
            )[side]
            table.append(
                pltpu.make_async_remote_copy(
                    src_ref=src, dst_ref=dst, send_sem=send_sem.at[e, side],
                    recv_sem=recv_sem.at[e, side], device_id=target, device_id_type=mesh_type,
                )
            )
        return table

    pending = []

    def send(e, source, firsts, lasts, ends=(0, 1, 2, 3)):
        colsend[e, 0] = firsts
        colsend[e, 1] = lasts
        table = copies(e, source, ends)
        for copy in table:
            copy.start()
        pending.extend(table)
        return table

    def receive(table):
        for copy in table:
            copy.wait_recv()

    thresh = LAMBDA / MU
    thresh_tv = LAMBDA_TV / MU

    def gradients(k, in_flight, last):
        e = 2 * (k - 1) + 1
        receive(in_flight)
        source = w3.at[k - 1]
        first_time = k == 1
        pl_left = None if last else colbuf[e, 0]
        pl_right = colbuf[e, 1]
        if not last:
            grad = colsend[e, 0] - pl_left
            ghost = grad if first_time else grad - d4c[...]
            clipped = jnp.clip(ghost, -thresh_tv, thresh_tv)
            d4c[...] = -clipped
            ghost_h = ghost - 2.0 * clipped

        def body(i, at, carry):
            primal, dual, firsts, lasts = carry
            rs = pl.ds(at, CH)
            x = [source[rs, lanes(r)] for r in range(rows)]
            below = rowbuf[e, 1, rs, :]
            if not last:
                above = rowbuf[e, 0, rs, :]
                ghost_v = x[0] - above
                if not first_time:
                    ghost_v = ghost_v - d4g[rs, :]
                cut = jnp.clip(ghost_v, -thresh_tv, thresh_tv)
                d4g[rs, :] = -cut
                over = ghost_v - 2.0 * cut
            results = []
            for r in range(rows):
                nxt = x[r + 1] if r + 1 < rows else below
                x_right = from_right(i, r, x[r], pl_right)
                sums = []
                for grad_now, v_ref, d_ref in (
                    (x_right - x[r], v4h, d4h), (nxt - x[r], v4v, d4v),
                ):
                    u = grad_now if first_time else grad_now - d_ref[rs, lanes(r)]
                    cut = jnp.clip(u, -thresh_tv, thresh_tv)
                    new = u - cut
                    res = cut if first_time else d_ref[rs, lanes(r)] + cut
                    change = new if first_time else new - v_ref[rs, lanes(r)]
                    primal = primal + fold(res * res)
                    dual = dual + fold(change * change)
                    if not last:
                        d_ref[rs, lanes(r)] = -cut
                        v_ref[rs, lanes(r)] = new
                        sums.append(new - cut)
                if not last:
                    x_left = from_left(i, r, x[r], pl_left)
                    h_left = from_left(i, r, sums[0], ghost_h)
                    back = (h_left - sums[0]) + (over - sums[1])
                    over = sums[1]
                    total = abun[rs, lanes(r)] - d3[rs, lanes(r)] + back
                    rhs[rs, lanes(r)] = total
                    prv = x[r - 1] if r else above
                    new_w = (total + ((prv + nxt) + (x_left + x_right))) * 0.2
                    w1[k, rs, lanes(r)] = new_w
                    results.append(new_w)
            if not last:
                firsts, lasts = pack(i, results, firsts, lasts)
            return primal, dual, firsts, lasts

        return chunks(endm, body, (zero, zero, zero, zero))

    def first_sweep(i, at, carry):
        rs = pl.ds(at, CH)
        results = []
        for r in range(rows):
            value = abun[rs, lanes(r)] * 0.2
            w1[0, rs, lanes(r)] = value
            results.append(value)
        return pack(i, results, *carry)

    def data_terms(first_time, last):
        def body(i, at, carry):
            primal, dual = carry
            rs = pl.ds(at, CH)
            for r in range(rows):
                old = d1[rs, lanes(r)]
                u = image[rs, lanes(r)] - old
                new = (spec_ref[rs, r, :] + MU * u) / (1.0 + MU)
                d_new = new - u
                res = old - d_new
                change = new - v1[rs, lanes(r)]
                primal = primal + fold(res * res)
                dual = dual + fold(change * change)
                if not last:
                    d1[rs, lanes(r)] = d_new
                    v1[rs, lanes(r)] = new
                    put_rhs(at, r, new + d_new)
            return primal, dual

        return body

    def point_terms(first_time, last):
        def body(i, at, carry):
            primal, dual = carry
            rs = pl.ds(at, CH)
            for r in range(rows):
                a = abun[rs, lanes(r)]
                old2 = None if first_time else d2[rs, lanes(r)]
                u2 = a if first_time else a - old2
                cut = jnp.clip(u2, -thresh, thresh)
                new2 = u2 - cut
                res2 = cut if first_time else old2 + cut
                change2 = new2 if first_time else new2 - v2[rs, lanes(r)]
                old5 = None if first_time else d5[rs, lanes(r)]
                u5 = a if first_time else a - old5
                new5 = jnp.maximum(u5, 0.0)
                res5 = a - new5
                change5 = new5 if first_time else new5 - v5[rs, lanes(r)]
                primal = primal + fold(res2 * res2 + res5 * res5)
                dual = dual + fold(change2 * change2 + change5 * change5)
                if last:
                    out_ref[rs, r, :] = a
                else:
                    d2[rs, lanes(r)] = -cut
                    v2[rs, lanes(r)] = new2
                    v5[rs, lanes(r)] = new5
                    d5[rs, lanes(r)] = new5 - u5
                    mixed[rs, lanes(r)] = mixed[rs, lanes(r)] + ((new2 - cut) + jnp.abs(u5))
            return primal, dual

        return body

    def second_sweep(k, last):
        e = 2 * k
        source = w1.at[k]
        first_time = k == 0
        pl_left = colbuf[e, 0]
        pl_right = colbuf[e, 1]

        def body(i, at, carry):
            primal, dual, firsts, lasts = carry
            rs = pl.ds(at, CH)
            x = [source[rs, lanes(r)] for r in range(rows)]
            above = rowbuf[e, 0, rs, :]
            below = rowbuf[e, 1, rs, :]
            results = []
            for r in range(rows):
                nxt = x[r + 1] if r + 1 < rows else below
                prv = x[r - 1] if r else above
                near = (prv + nxt) + (
                    from_left(i, r, x[r], pl_left) + from_right(i, r, x[r], pl_right)
                )
                a = abun[rs, lanes(r)]
                total = a if first_time else rhs[rs, lanes(r)]
                new = (total + near) * 0.2
                w3[k, rs, lanes(r)] = new
                results.append(new)
                res = a - new
                change = new if first_time else new - w3[k - 1, rs, lanes(r)]
                primal = primal + fold(res * res)
                dual = dual + fold(change * change)
                if not last:
                    d_new = new - a if first_time else new - (a - d3[rs, lanes(r)])
                    d3[rs, lanes(r)] = d_new
                    put_rhs(at, r, mixed[rs, lanes(r)] + (new + d_new))
            firsts, lasts = pack(i, results, firsts, lasts)
            return primal, dual, firsts, lasts

        return chunks(endm, body, (zero, zero, zero, zero))

    table = None
    partial = [[zero, zero] for _ in range(ITERS)]

    def add(k, pair):
        partial[k][0] = partial[k][0] + pair[0]
        partial[k][1] = partial[k][1] + pair[1]

    for k in range(ITERS):
        last = k == ITERS - 1
        abun[...] = dot(inv3[...], rhs3[...])
        if k == 0:
            firsts, lasts = chunks(endm, first_sweep, (zero, zero))
        else:
            primal, dual, firsts, lasts = gradients(k, table, False)
            add(k - 1, (primal, dual))
        table = send(2 * k, w1.at[k], firsts, lasts)

        def put_abun(i, at, carry):
            for r in range(rows):
                put_rhs(at, r, abun[pl.ds(at, CH), lanes(r)])
            return carry

        chunks(endm, put_abun, 0)
        image[...] = dot(lib3[...], rhs3[...])
        add(k, chunks(bands, data_terms(k == 0, last), (zero, zero)))
        if not last:
            for base in (0, pad, 2 * pad):
                rhs3[base + bands : base + endm, :] = jnp.zeros((endm - bands, rows * cols), BF16)
            mixed[...] = dot(libt3[...], rhs3[...])
        add(k, chunks(endm, point_terms(k == 0, last), (zero, zero)))
        receive(table)
        primal, dual, firsts, lasts = second_sweep(k, last)
        add(k, (primal, dual))
        table = send(2 * k + 1, w3.at[k], firsts, lasts, (1, 3) if last else (0, 1, 2, 3))
    add(ITERS - 1, gradients(ITERS, table, True)[:2])

    def gather(stage, value, index, peers, slots):
        slots[index] = value
        summing[stage] = value
        table = [
            pltpu.make_async_remote_copy(
                src_ref=summing.at[stage], dst_ref=slots.at[index],
                send_sem=sum_send.at[stage, i], recv_sem=sum_recv.at[stage, i],
                device_id=peer, device_id_type=mesh_type,
            )
            for i, peer in enumerate(peers)
        ]
        for copy in table:
            copy.start()
        pending.extend(table)
        for copy in table:
            copy.wait_recv()
        total = slots[0]
        for i in range(1, len(peers) + 1):
            total = total + slots[i]
        return total

    sums = [jnp.sum(partial[k][0], axis=0, keepdims=True) for k in range(ITERS)]
    sums += [jnp.sum(partial[k][1], axis=0, keepdims=True) * (MU * MU) for k in range(ITERS)]
    totals = gather(0, jnp.concatenate(sums, axis=0), me_r, row_peers, row_slots)
    totals = gather(1, totals, me_c, col_peers, col_slots)
    numel = float(endm * rows * cols * n_rows * n_cols)
    final = jnp.sqrt(jnp.sum(totals, axis=1, keepdims=True) / numel)
    norm_ref[:, 0:1] = final[0:ITERS]
    norm_ref[:, 1:2] = final[ITERS : 2 * ITERS]
    for copy in pending:
        copy.wait_send()


def local(spectra, library):
    bands, rows, cols = spectra.shape
    endm = library.shape[1]
    n_rows, n_cols = lax.axis_size("rows"), lax.axis_size("cols")
    pad = -(-max(bands, endm) // 256) * 256
    lib = jnp.pad(library, ((0, pad - bands), (0, pad - endm)))
    wide = rows * cols
    dims = (bands, endm, rows, cols, n_rows, n_cols, pad)
    field = pltpu.VMEM((endm, wide), F32)
    full = pltpu.VMEM((pad, wide), F32)
    band = pltpu.VMEM((bands, wide), F32)
    square = pltpu.VMEM((pad, pad), F32)
    stacked = pltpu.VMEM((pad, 3 * pad), BF16)
    exchanges = 2 * ITERS
    abundance, norms = pl.pallas_call(
        functools.partial(kernel, dims),
        out_shape=(
            jax.ShapeDtypeStruct((endm, rows, cols), F32),
            jax.ShapeDtypeStruct((ITERS, 2), F32),
        ),
        in_specs=[pl.BlockSpec(memory_space=pltpu.VMEM)] * 3,
        out_specs=(pl.BlockSpec(memory_space=pltpu.VMEM),) * 2,
        scratch_shapes=[
            stacked, stacked, stacked, pltpu.VMEM((3 * pad, wide), BF16),
            square, square, square,
            full, full, full, field, band, band, field, field, field, field, field,
            field, field, field, field, pltpu.VMEM((endm, cols), F32), pltpu.VMEM((8, cols), F32),
            pltpu.VMEM((ITERS, endm, wide), F32), pltpu.VMEM((ITERS, endm, wide), F32),
            pltpu.VMEM((exchanges, 2, endm, cols), F32),
            pltpu.VMEM((exchanges, 2, 8, cols), F32),
            pltpu.VMEM((exchanges, 2, 8, cols), F32),
            pltpu.SemaphoreType.DMA((exchanges, 4)),
            pltpu.SemaphoreType.DMA((exchanges, 4)),
            pltpu.VMEM((2, 8, cols), F32),
            pltpu.VMEM((n_rows, 8, cols), F32),
            pltpu.VMEM((n_cols, 8, cols), F32),
            pltpu.SemaphoreType.DMA((2, max(n_rows, n_cols))),
            pltpu.SemaphoreType.DMA((2, max(n_rows, n_cols))),
        ],
        compiler_params=pltpu.CompilerParams(
            collective_id=0, has_side_effects=True, vmem_limit_bytes=56 * 1024 * 1024
        ),
    )(spectra, lib, lib.T)
    return abundance, norms


def solution(mesh):
    placed = (P(None, "rows", "cols"), P())
    return jax.shard_map(
        local, mesh=mesh, in_specs=placed, out_specs=(P(None, "rows", "cols"), P()), check_vma=False
    )
```

```python
import functools

import jax
import jax.numpy as jnp
from jax import lax
from jax.experimental import pallas as pl
from jax.experimental.pallas import tpu as pltpu
from jax.sharding import PartitionSpec as P

ITERS = 4
MU = 0.5
LAMBDA = 0.02
LAMBDA_TV = 0.05
SHIFT = 3.0
NEWTON = 8
CH = 16
F32 = jnp.float32
BF16 = jnp.bfloat16


def split(value):
    high = value.astype(BF16)
    return high, (value - high.astype(F32)).astype(BF16)


def dot(lhs, rhs):
    return jnp.dot(lhs, rhs, preferred_element_type=F32)


def dot_full(lhs, rhs):
    return jnp.dot(lhs, rhs, precision=lax.Precision.HIGHEST, preferred_element_type=F32)


def kernel(
    dims, spec_ref, lib_ref, out_ref, norm_ref,
    inv3, lib3, libt3, rhs3, newton_x, newton_r, gram,
    abun, image, mixed, rhs, v1, d1, v2, d2, v5, d5, d3, v4h, d4h, v4v, d4v, d4g, d4c,
    w1, w3, rowbuf, colbuf, colsend, send_sem, recv_sem,
    summing, row_slots, col_slots, sum_send, sum_recv,
):
    bands, endm, rows, cols, n_rows, n_cols, pad = dims
    me_r, me_c = lax.axis_index("rows"), lax.axis_index("cols")
    up = (lax.rem(me_r + n_rows - 1, n_rows), me_c)
    down = (lax.rem(me_r + 1, n_rows), me_c)
    left = (me_r, lax.rem(me_c + n_cols - 1, n_cols))
    right = (me_r, lax.rem(me_c + 1, n_cols))
    mesh_type = pl.DeviceIdType.MESH
    barrier = pltpu.get_barrier_semaphore()
    row_peers = [(lax.rem(me_r + step, n_rows), me_c) for step in range(1, n_rows)]
    col_peers = [(me_r, lax.rem(me_c + step, n_cols)) for step in range(1, n_cols)]
    for target in row_peers + col_peers:
        pl.semaphore_signal(barrier, inc=1, device_id=target, device_id_type=mesh_type)

    lane = lax.broadcasted_iota(jnp.int32, (8, cols), 1)

    def lanes(r):
        return slice(r * cols, (r + 1) * cols)

    def stack_lhs(ref, value):
        high, low = split(value)
        ref[:, 0:pad] = high
        ref[:, pad : 2 * pad] = high
        ref[:, 2 * pad : 3 * pad] = low

    def put_rhs(at, r, value):
        high, low = split(value)
        rhs3[pl.ds(at, CH), lanes(r)] = high
        rhs3[pl.ds(at + pad, CH), lanes(r)] = low
        rhs3[pl.ds(at + 2 * pad, CH), lanes(r)] = high

    def fold(value):
        total = value[0:8]
        for i in range(8, CH, 8):
            total = total + value[i : i + 8]
        return total

    def chunks(count, body, init, base=0):
        def step(i, carry):
            return body(i, pl.multiple_of(i * CH + base, CH), carry)

        return lax.fori_loop(0, count // CH, step, init)

    zero = jnp.zeros((8, cols), F32)
    middle = (endm // CH + 1) // 2 * CH
    parts = ((0, middle), (middle, endm - middle))

    def load_spectra(i, at, carry):
        for r in range(rows):
            value = spec_ref[pl.ds(at, CH), r, :]
            v1[pl.ds(at, CH), lanes(r)] = value
            d1[pl.ds(at, CH), lanes(r)] = jnp.zeros((CH, cols), F32)
            put_rhs(at, r, value)
        return carry

    for base in (0, pad, 2 * pad):
        rhs3[base + bands : base + pad, :] = jnp.zeros((pad - bands, rows * cols), BF16)
    chunks(bands, load_spectra, 0)

    newton_r[...] = jnp.zeros((pad, pad), F32)
    newton_r[0:bands, 0:endm] = lib_ref[...]
    newton_x[...] = newton_r[...].T
    stack_lhs(lib3, newton_r[...])
    stack_lhs(libt3, newton_x[...])
    mixed[...] = dot(libt3[...], rhs3[...])
    eye = (
        lax.broadcasted_iota(jnp.int32, (pad, pad), 0)
        == lax.broadcasted_iota(jnp.int32, (pad, pad), 1)
    ).astype(F32)
    gram[...] = dot_full(newton_x[...], newton_r[...]) + SHIFT * eye
    bound = jnp.max(jnp.sum(jnp.abs(gram[...]), axis=1, keepdims=True), axis=0, keepdims=True)
    scale = 2.0 / (SHIFT + bound)
    newton_x[...] = eye * scale
    newton_r[...] = eye - gram[...] * scale

    def newton(_, radius):
        square = radius * radius
        factor = 2.0 / (2.0 - square)
        r_val = newton_r[...]
        x_val = newton_x[...]
        r_hi, r_lo = split(r_val)
        x_hi, x_lo = split(x_val)
        r_next = dot(r_hi, r_hi) + dot(r_hi, r_lo) + dot(r_lo, r_hi)
        x_next = dot(x_hi, r_hi) + dot(x_hi, r_lo) + dot(x_lo, r_hi)
        newton_x[...] = factor * (x_val + x_next)
        newton_r[...] = (1.0 - factor) * eye + factor * r_next
        return square / (2.0 - square)

    lax.fori_loop(0, NEWTON, newton, (bound - SHIFT) / (bound + SHIFT))
    for _ in range(2):
        newton_r[...] = eye - dot_full(gram[...], newton_x[...])
        newton_x[...] = newton_x[...] + dot_full(newton_x[...], newton_r[...])
    stack_lhs(inv3, newton_x[...])

    def put_mixed(i, at, carry):
        for r in range(rows):
            put_rhs(at, r, mixed[pl.ds(at, CH), lanes(r)])
        return carry

    for base in (0, pad, 2 * pad):
        rhs3[base + endm : base + pad, :] = jnp.zeros((pad - endm, rows * cols), BF16)
    chunks(endm, put_mixed, 0)
    pl.semaphore_wait(barrier, n_rows + n_cols - 2)

    def pack(i, values, firsts, lasts):
        for half in range(CH // 8):
            for r in range(rows):
                spot = (i * (CH // 8) + half) * rows + r
                part = values[r][8 * half : 8 * half + 8]
                hit = lane == spot
                firsts = jnp.where(hit, pltpu.roll(part, spot, 1), firsts)
                lasts = jnp.where(hit, pltpu.roll(part, lax.rem(spot + 1, cols), 1), lasts)
        return firsts, lasts

    def unpack(i, r, packed, spot_to):
        parts = []
        for half in range(CH // 8):
            spot = (i * (CH // 8) + half) * rows + r
            parts.append(pltpu.roll(packed, lax.rem(spot_to - spot + cols, cols), 1))
        return jnp.concatenate(parts, axis=0)

    wide_lane = lax.broadcasted_iota(jnp.int32, (CH, cols), 1)

    def from_left(i, r, value, packed):
        return jnp.where(wide_lane == 0, unpack(i, r, packed, 0), pltpu.roll(value, 1, 1))

    def from_right(i, r, value, packed):
        return jnp.where(
            wide_lane == cols - 1, unpack(i, r, packed, cols - 1), pltpu.roll(value, cols - 1, 1)
        )

    def copies(e, half, source, ends):
        table = []
        span = pl.ds(*parts[half])
        for side in ends:
            src, dst, target = (
                (source.at[span, lanes(rows - 1)], rowbuf.at[e, 0, span], down),
                (source.at[span, lanes(0)], rowbuf.at[e, 1, span], up),
                (colsend.at[e, half, 1], colbuf.at[e, half, 0], right),
                (colsend.at[e, half, 0], colbuf.at[e, half, 1], left),
            )[side]
            table.append(
                pltpu.make_async_remote_copy(
                    src_ref=src, dst_ref=dst, send_sem=send_sem.at[e, half, side],
                    recv_sem=recv_sem.at[e, half, side], device_id=target, device_id_type=mesh_type,
                )
            )
        return table

    pending = []

    def send(e, half, source, firsts, lasts, ends=(0, 1, 2, 3)):
        colsend[e, half, 0] = firsts
        colsend[e, half, 1] = lasts
        table = copies(e, half, source, ends)
        for copy in table:
            copy.start()
        pending.extend(table)
        return table

    def receive(table):
        for copy in table:
            copy.wait_recv()

    thresh = LAMBDA / MU
    thresh_tv = LAMBDA_TV / MU

    def gradients(k, half, in_flight, last):
        e = 2 * (k - 1) + 1
        receive(in_flight)
        source = w3.at[k - 1]
        first_time = k == 1
        pl_left = None if last else colbuf[e, half, 0]
        pl_right = colbuf[e, half, 1]
        if not last:
            grad = colsend[e, half, 0] - pl_left
            ghost = grad if first_time else grad - d4c[half]
            clipped = jnp.clip(ghost, -thresh_tv, thresh_tv)
            d4c[half] = -clipped
            ghost_h = ghost - 2.0 * clipped

        def body(i, at, carry):
            primal, dual, firsts, lasts = carry
            rs = pl.ds(at, CH)
            x = [source[rs, lanes(r)] for r in range(rows)]
            below = rowbuf[e, 1, rs, :]
            if not last:
                above = rowbuf[e, 0, rs, :]
                ghost_v = x[0] - above
                if not first_time:
                    ghost_v = ghost_v - d4g[rs, :]
                cut = jnp.clip(ghost_v, -thresh_tv, thresh_tv)
                d4g[rs, :] = -cut
                over = ghost_v - 2.0 * cut
            results = []
            for r in range(rows):
                nxt = x[r + 1] if r + 1 < rows else below
                x_right = from_right(i, r, x[r], pl_right)
                sums = []
                for grad_now, v_ref, d_ref in (
                    (x_right - x[r], v4h, d4h), (nxt - x[r], v4v, d4v),
                ):
                    u = grad_now if first_time else grad_now - d_ref[rs, lanes(r)]
                    cut = jnp.clip(u, -thresh_tv, thresh_tv)
                    new = u - cut
                    res = cut if first_time else d_ref[rs, lanes(r)] + cut
                    change = new if first_time else new - v_ref[rs, lanes(r)]
                    primal = primal + fold(res * res)
                    dual = dual + fold(change * change)
                    if not last:
                        d_ref[rs, lanes(r)] = -cut
                        v_ref[rs, lanes(r)] = new
                        sums.append(new - cut)
                if not last:
                    x_left = from_left(i, r, x[r], pl_left)
                    h_left = from_left(i, r, sums[0], ghost_h)
                    back = (h_left - sums[0]) + (over - sums[1])
                    over = sums[1]
                    total = abun[rs, lanes(r)] - d3[rs, lanes(r)] + back
                    rhs[rs, lanes(r)] = total
                    prv = x[r - 1] if r else above
                    new_w = (total + ((prv + nxt) + (x_left + x_right))) * 0.2
                    w1[k, rs, lanes(r)] = new_w
                    results.append(new_w)
            if not last:
                firsts, lasts = pack(i, results, firsts, lasts)
            return primal, dual, firsts, lasts

        return chunks(parts[half][1], body, (zero, zero, zero, zero), parts[half][0])

    def first_sweep(i, at, carry):
        rs = pl.ds(at, CH)
        results = []
        for r in range(rows):
            value = abun[rs, lanes(r)] * 0.2
            w1[0, rs, lanes(r)] = value
            results.append(value)
        return pack(i, results, *carry)

    def data_terms(first_time, last):
        def body(i, at, carry):
            primal, dual = carry
            rs = pl.ds(at, CH)
            for r in range(rows):
                old = d1[rs, lanes(r)]
                u = image[rs, lanes(r)] - old
                new = (spec_ref[rs, r, :] + MU * u) / (1.0 + MU)
                d_new = new - u
                res = old - d_new
                change = new - v1[rs, lanes(r)]
                primal = primal + fold(res * res)
                dual = dual + fold(change * change)
                if not last:
                    d1[rs, lanes(r)] = d_new
                    v1[rs, lanes(r)] = new
                    put_rhs(at, r, new + d_new)
            return primal, dual

        return body

    def point_terms(first_time, last):
        def body(i, at, carry):
            primal, dual = carry
            rs = pl.ds(at, CH)
            for r in range(rows):
                a = abun[rs, lanes(r)]
                old2 = None if first_time else d2[rs, lanes(r)]
                u2 = a if first_time else a - old2
                cut = jnp.clip(u2, -thresh, thresh)
                new2 = u2 - cut
                res2 = cut if first_time else old2 + cut
                change2 = new2 if first_time else new2 - v2[rs, lanes(r)]
                old5 = None if first_time else d5[rs, lanes(r)]
                u5 = a if first_time else a - old5
                new5 = jnp.maximum(u5, 0.0)
                res5 = a - new5
                change5 = new5 if first_time else new5 - v5[rs, lanes(r)]
                primal = primal + fold(res2 * res2 + res5 * res5)
                dual = dual + fold(change2 * change2 + change5 * change5)
                if last:
                    out_ref[rs, r, :] = a
                else:
                    d2[rs, lanes(r)] = -cut
                    v2[rs, lanes(r)] = new2
                    v5[rs, lanes(r)] = new5
                    d5[rs, lanes(r)] = new5 - u5
                    mixed[rs, lanes(r)] = mixed[rs, lanes(r)] + ((new2 - cut) + jnp.abs(u5))
            return primal, dual

        return body

    def second_sweep(k, half, last):
        e = 2 * k
        source = w1.at[k]
        first_time = k == 0
        pl_left = colbuf[e, half, 0]
        pl_right = colbuf[e, half, 1]

        def body(i, at, carry):
            primal, dual, firsts, lasts = carry
            rs = pl.ds(at, CH)
            x = [source[rs, lanes(r)] for r in range(rows)]
            above = rowbuf[e, 0, rs, :]
            below = rowbuf[e, 1, rs, :]
            results = []
            for r in range(rows):
                nxt = x[r + 1] if r + 1 < rows else below
                prv = x[r - 1] if r else above
                near = (prv + nxt) + (
                    from_left(i, r, x[r], pl_left) + from_right(i, r, x[r], pl_right)
                )
                a = abun[rs, lanes(r)]
                total = a if first_time else rhs[rs, lanes(r)]
                new = (total + near) * 0.2
                w3[k, rs, lanes(r)] = new
                results.append(new)
                res = a - new
                change = new if first_time else new - w3[k - 1, rs, lanes(r)]
                primal = primal + fold(res * res)
                dual = dual + fold(change * change)
                if not last:
                    d_new = new - a if first_time else new - (a - d3[rs, lanes(r)])
                    d3[rs, lanes(r)] = d_new
                    put_rhs(at, r, mixed[rs, lanes(r)] + (new + d_new))
            firsts, lasts = pack(i, results, firsts, lasts)
            return primal, dual, firsts, lasts

        return chunks(parts[half][1], body, (zero, zero, zero, zero), parts[half][0])

    tables = [None, None]
    partial = [[zero, zero] for _ in range(ITERS)]

    def add(k, pair):
        partial[k][0] = partial[k][0] + pair[0]
        partial[k][1] = partial[k][1] + pair[1]

    def put_abun(i, at, carry):
        for r in range(rows):
            put_rhs(at, r, abun[pl.ds(at, CH), lanes(r)])
        return carry

    def image_terms(k, last):
        chunks(endm, put_abun, 0)
        image[...] = dot(lib3[...], rhs3[...])
        add(k, chunks(bands, data_terms(k == 0, last), (zero, zero)))

    for k in range(ITERS):
        last = k == ITERS - 1
        abun[...] = dot(inv3[...], rhs3[...])
        if k:
            image_terms(k, last)
        for half in range(2):
            if k == 0:
                firsts, lasts = chunks(parts[half][1], first_sweep, (zero, zero), parts[half][0])
            else:
                primal, dual, firsts, lasts = gradients(k, half, tables[half], False)
                add(k - 1, (primal, dual))
            tables[half] = send(2 * k, half, w1.at[k], firsts, lasts)
        if k == 0:
            image_terms(k, last)
        if not last:
            mixed[...] = dot(libt3[...], rhs3[...])
        add(k, chunks(endm, point_terms(k == 0, last), (zero, zero)))
        for half in range(2):
            receive(tables[half])
            primal, dual, firsts, lasts = second_sweep(k, half, last)
            add(k, (primal, dual))
            ends = (1, 3) if last else (0, 1, 2, 3)
            tables[half] = send(2 * k + 1, half, w3.at[k], firsts, lasts, ends)
    for half in range(2):
        add(ITERS - 1, gradients(ITERS, half, tables[half], True)[:2])

    def gather(stage, value, index, peers, slots):
        slots[index] = value
        summing[stage] = value
        table = [
            pltpu.make_async_remote_copy(
                src_ref=summing.at[stage], dst_ref=slots.at[index],
                send_sem=sum_send.at[stage, i], recv_sem=sum_recv.at[stage, i],
                device_id=peer, device_id_type=mesh_type,
            )
            for i, peer in enumerate(peers)
        ]
        for copy in table:
            copy.start()
        pending.extend(table)
        for copy in table:
            copy.wait_recv()
        total = slots[0]
        for i in range(1, len(peers) + 1):
            total = total + slots[i]
        return total

    sums = [jnp.sum(partial[k][0], axis=0, keepdims=True) for k in range(ITERS)]
    sums += [jnp.sum(partial[k][1], axis=0, keepdims=True) * (MU * MU) for k in range(ITERS)]
    totals = gather(0, jnp.concatenate(sums, axis=0), me_r, row_peers, row_slots)
    totals = gather(1, totals, me_c, col_peers, col_slots)
    numel = float(endm * rows * cols * n_rows * n_cols)
    final = jnp.sqrt(jnp.sum(totals, axis=1, keepdims=True) / numel)
    norm_ref[:, 0:1] = final[0:ITERS]
    norm_ref[:, 1:2] = final[ITERS : 2 * ITERS]
    for copy in pending:
        copy.wait_send()


def local(spectra, library):
    bands, rows, cols = spectra.shape
    endm = library.shape[1]
    n_rows, n_cols = lax.axis_size("rows"), lax.axis_size("cols")
    pad = -(-max(bands, endm) // 256) * 256
    wide = rows * cols
    dims = (bands, endm, rows, cols, n_rows, n_cols, pad)
    field = pltpu.VMEM((endm, wide), F32)
    full = pltpu.VMEM((pad, wide), F32)
    band = pltpu.VMEM((bands, wide), F32)
    square = pltpu.VMEM((pad, pad), F32)
    stacked = pltpu.VMEM((pad, 3 * pad), BF16)
    exchanges = 2 * ITERS
    abundance, norms = pl.pallas_call(
        functools.partial(kernel, dims),
        out_shape=(
            jax.ShapeDtypeStruct((endm, rows, cols), F32),
            jax.ShapeDtypeStruct((ITERS, 2), F32),
        ),
        in_specs=[pl.BlockSpec(memory_space=pltpu.VMEM)] * 2,
        out_specs=(pl.BlockSpec(memory_space=pltpu.VMEM),) * 2,
        scratch_shapes=[
            stacked, stacked, stacked, pltpu.VMEM((3 * pad, wide), BF16),
            square, square, square,
            full, full, full, field, band, band, field, field, field, field, field,
            field, field, field, field, pltpu.VMEM((endm, cols), F32), pltpu.VMEM((2, 8, cols), F32),
            pltpu.VMEM((ITERS, endm, wide), F32), pltpu.VMEM((ITERS, endm, wide), F32),
            pltpu.VMEM((exchanges, 2, endm, cols), F32),
            pltpu.VMEM((exchanges, 2, 2, 8, cols), F32),
            pltpu.VMEM((exchanges, 2, 2, 8, cols), F32),
            pltpu.SemaphoreType.DMA((exchanges, 2, 4)),
            pltpu.SemaphoreType.DMA((exchanges, 2, 4)),
            pltpu.VMEM((2, 8, cols), F32),
            pltpu.VMEM((n_rows, 8, cols), F32),
            pltpu.VMEM((n_cols, 8, cols), F32),
            pltpu.SemaphoreType.DMA((2, max(n_rows, n_cols))),
            pltpu.SemaphoreType.DMA((2, max(n_rows, n_cols))),
        ],
        compiler_params=pltpu.CompilerParams(
            collective_id=0, has_side_effects=True, vmem_limit_bytes=56 * 1024 * 1024
        ),
    )(spectra, library)
    return abundance, norms


def solution(mesh):
    placed = (P(None, "rows", "cols"), P())
    return jax.shard_map(
        local, mesh=mesh, in_specs=placed, out_specs=(P(None, "rows", "cols"), P()), check_vma=False
    )
```

```python
import functools

import jax
import jax.numpy as jnp
from jax import lax
from jax.experimental import pallas as pl
from jax.experimental.pallas import tpu as pltpu
from jax.sharding import PartitionSpec as P

ITERS = 4
MU = 0.5
LAMBDA = 0.02
LAMBDA_TV = 0.05
SHIFT = 3.0
NEWTON = 8
CH = 16
PARTS = 5
F32 = jnp.float32
BF16 = jnp.bfloat16


def split(value):
    high = value.astype(BF16)
    return high, (value - high.astype(F32)).astype(BF16)


def dot(lhs, rhs):
    return jnp.dot(lhs, rhs, preferred_element_type=F32)


def dot_full(lhs, rhs):
    return jnp.dot(lhs, rhs, precision=lax.Precision.HIGHEST, preferred_element_type=F32)


def kernel(
    dims, spec_ref, lib_ref, out_ref, norm_ref,
    inv3, lib3, libt3, rhs3, newton_x, newton_r, gram,
    abun, image, mixed, rhs, v1, d1, v2, d2, v5, d5, d3, v4h, d4h, v4v, d4v, d4g, d4c,
    w1, w3, rowbuf, colbuf, colsend, send_sem, recv_sem,
    summing, row_slots, col_slots, sum_send, sum_recv,
):
    bands, endm, rows, cols, n_rows, n_cols, pad = dims
    me_r, me_c = lax.axis_index("rows"), lax.axis_index("cols")
    up = (lax.rem(me_r + n_rows - 1, n_rows), me_c)
    down = (lax.rem(me_r + 1, n_rows), me_c)
    left = (me_r, lax.rem(me_c + n_cols - 1, n_cols))
    right = (me_r, lax.rem(me_c + 1, n_cols))
    mesh_type = pl.DeviceIdType.MESH
    barrier = pltpu.get_barrier_semaphore()
    row_peers = [(lax.rem(me_r + step, n_rows), me_c) for step in range(1, n_rows)]
    col_peers = [(me_r, lax.rem(me_c + step, n_cols)) for step in range(1, n_cols)]
    for target in row_peers + col_peers:
        pl.semaphore_signal(barrier, inc=1, device_id=target, device_id_type=mesh_type)

    lane = lax.broadcasted_iota(jnp.int32, (8, cols), 1)

    def lanes(r):
        return slice(r * cols, (r + 1) * cols)

    def stack_lhs(ref, value):
        high, low = split(value)
        ref[:, 0:pad] = high
        ref[:, pad : 2 * pad] = high
        ref[:, 2 * pad : 3 * pad] = low

    def put_rhs(at, r, value):
        high, low = split(value)
        rhs3[pl.ds(at, CH), lanes(r)] = high
        rhs3[pl.ds(at + pad, CH), lanes(r)] = low
        rhs3[pl.ds(at + 2 * pad, CH), lanes(r)] = high

    def fold(value):
        total = value[0:8]
        for i in range(8, CH, 8):
            total = total + value[i : i + 8]
        return total

    def chunks(count, body, init, base=0):
        def step(i, carry):
            return body(i, pl.multiple_of(i * CH + base, CH), carry)

        return lax.fori_loop(0, count // CH, step, init)

    zero = jnp.zeros((8, cols), F32)
    edges = [endm // CH * i // PARTS * CH for i in range(PARTS + 1)]
    parts = [(lo, hi - lo) for lo, hi in zip(edges[:-1], edges[1:])]

    def load_spectra(i, at, carry):
        for r in range(rows):
            value = spec_ref[pl.ds(at, CH), r, :]
            v1[pl.ds(at, CH), lanes(r)] = value
            d1[pl.ds(at, CH), lanes(r)] = jnp.zeros((CH, cols), F32)
            put_rhs(at, r, value)
        return carry

    for base in (0, pad, 2 * pad):
        rhs3[base + bands : base + pad, :] = jnp.zeros((pad - bands, rows * cols), BF16)
    chunks(bands, load_spectra, 0)

    newton_r[...] = jnp.zeros((pad, pad), F32)
    newton_r[0:bands, 0:endm] = lib_ref[...]
    newton_x[...] = newton_r[...].T
    stack_lhs(lib3, newton_r[...])
    stack_lhs(libt3, newton_x[...])
    mixed[...] = dot(libt3[...], rhs3[...])
    eye = (
        lax.broadcasted_iota(jnp.int32, (pad, pad), 0)
        == lax.broadcasted_iota(jnp.int32, (pad, pad), 1)
    ).astype(F32)
    gram[...] = dot_full(newton_x[...], newton_r[...]) + SHIFT * eye
    bound = jnp.max(jnp.sum(jnp.abs(gram[...]), axis=1, keepdims=True), axis=0, keepdims=True)
    scale = 2.0 / (SHIFT + bound)
    newton_x[...] = eye * scale
    newton_r[...] = eye - gram[...] * scale

    def newton(_, radius):
        square = radius * radius
        factor = 2.0 / (2.0 - square)
        r_val = newton_r[...]
        x_val = newton_x[...]
        r_hi, r_lo = split(r_val)
        x_hi, x_lo = split(x_val)
        r_next = dot(r_hi, r_hi) + dot(r_hi, r_lo) + dot(r_lo, r_hi)
        x_next = dot(x_hi, r_hi) + dot(x_hi, r_lo) + dot(x_lo, r_hi)
        newton_x[...] = factor * (x_val + x_next)
        newton_r[...] = (1.0 - factor) * eye + factor * r_next
        return square / (2.0 - square)

    lax.fori_loop(0, NEWTON, newton, (bound - SHIFT) / (bound + SHIFT))
    for _ in range(2):
        newton_r[...] = eye - dot_full(gram[...], newton_x[...])
        newton_x[...] = newton_x[...] + dot_full(newton_x[...], newton_r[...])
    stack_lhs(inv3, newton_x[...])

    def put_mixed(i, at, carry):
        for r in range(rows):
            put_rhs(at, r, mixed[pl.ds(at, CH), lanes(r)])
        return carry

    for base in (0, pad, 2 * pad):
        rhs3[base + endm : base + pad, :] = jnp.zeros((pad - endm, rows * cols), BF16)
    chunks(endm, put_mixed, 0)
    pl.semaphore_wait(barrier, n_rows + n_cols - 2)

    def pack(i, values, firsts, lasts):
        for half in range(CH // 8):
            for r in range(rows):
                spot = (i * (CH // 8) + half) * rows + r
                part = values[r][8 * half : 8 * half + 8]
                hit = lane == spot
                firsts = jnp.where(hit, pltpu.roll(part, spot, 1), firsts)
                lasts = jnp.where(hit, pltpu.roll(part, lax.rem(spot + 1, cols), 1), lasts)
        return firsts, lasts

    def unpack(i, r, packed, spot_to):
        parts = []
        for half in range(CH // 8):
            spot = (i * (CH // 8) + half) * rows + r
            parts.append(pltpu.roll(packed, lax.rem(spot_to - spot + cols, cols), 1))
        return jnp.concatenate(parts, axis=0)

    wide_lane = lax.broadcasted_iota(jnp.int32, (CH, cols), 1)

    def from_left(i, r, value, packed):
        return jnp.where(wide_lane == 0, unpack(i, r, packed, 0), pltpu.roll(value, 1, 1))

    def from_right(i, r, value, packed):
        return jnp.where(
            wide_lane == cols - 1, unpack(i, r, packed, cols - 1), pltpu.roll(value, cols - 1, 1)
        )

    def copies(e, half, source, ends):
        table = []
        span = pl.ds(*parts[half])
        for side in ends:
            src, dst, target = (
                (source.at[span, lanes(rows - 1)], rowbuf.at[e, 0, span], down),
                (source.at[span, lanes(0)], rowbuf.at[e, 1, span], up),
                (colsend.at[e, half, 1], colbuf.at[e, half, 0], right),
                (colsend.at[e, half, 0], colbuf.at[e, half, 1], left),
            )[side]
            table.append(
                pltpu.make_async_remote_copy(
                    src_ref=src, dst_ref=dst, send_sem=send_sem.at[e, half, side],
                    recv_sem=recv_sem.at[e, half, side], device_id=target, device_id_type=mesh_type,
                )
            )
        return table

    pending = []

    def send(e, half, source, firsts, lasts, ends=(0, 1, 2, 3)):
        colsend[e, half, 0] = firsts
        colsend[e, half, 1] = lasts
        table = copies(e, half, source, ends)
        for copy in table:
            copy.start()
        pending.extend(table)
        return table

    def receive(table):
        for copy in table:
            copy.wait_recv()

    thresh = LAMBDA / MU
    thresh_tv = LAMBDA_TV / MU

    def gradients(k, half, in_flight, last):
        e = 2 * (k - 1) + 1
        receive(in_flight)
        source = w3.at[k - 1]
        first_time = k == 1
        pl_left = None if last else colbuf[e, half, 0]
        pl_right = colbuf[e, half, 1]
        if not last:
            grad = colsend[e, half, 0] - pl_left
            ghost = grad if first_time else grad - d4c[half]
            clipped = jnp.clip(ghost, -thresh_tv, thresh_tv)
            d4c[half] = -clipped
            ghost_h = ghost - 2.0 * clipped

        def body(i, at, carry):
            primal, dual, firsts, lasts = carry
            rs = pl.ds(at, CH)
            x = [source[rs, lanes(r)] for r in range(rows)]
            below = rowbuf[e, 1, rs, :]
            if not last:
                above = rowbuf[e, 0, rs, :]
                ghost_v = x[0] - above
                if not first_time:
                    ghost_v = ghost_v - d4g[rs, :]
                cut = jnp.clip(ghost_v, -thresh_tv, thresh_tv)
                d4g[rs, :] = -cut
                over = ghost_v - 2.0 * cut
            results = []
            for r in range(rows):
                nxt = x[r + 1] if r + 1 < rows else below
                x_right = from_right(i, r, x[r], pl_right)
                sums = []
                for grad_now, v_ref, d_ref in (
                    (x_right - x[r], v4h, d4h), (nxt - x[r], v4v, d4v),
                ):
                    u = grad_now if first_time else grad_now - d_ref[rs, lanes(r)]
                    cut = jnp.clip(u, -thresh_tv, thresh_tv)
                    new = u - cut
                    res = cut if first_time else d_ref[rs, lanes(r)] + cut
                    change = new if first_time else new - v_ref[rs, lanes(r)]
                    primal = primal + fold(res * res)
                    dual = dual + fold(change * change)
                    if not last:
                        d_ref[rs, lanes(r)] = -cut
                        v_ref[rs, lanes(r)] = new
                        sums.append(new - cut)
                if not last:
                    x_left = from_left(i, r, x[r], pl_left)
                    h_left = from_left(i, r, sums[0], ghost_h)
                    back = (h_left - sums[0]) + (over - sums[1])
                    over = sums[1]
                    total = abun[rs, lanes(r)] - d3[rs, lanes(r)] + back
                    rhs[rs, lanes(r)] = total
                    prv = x[r - 1] if r else above
                    new_w = (total + ((prv + nxt) + (x_left + x_right))) * 0.2
                    w1[k, rs, lanes(r)] = new_w
                    results.append(new_w)
            if not last:
                firsts, lasts = pack(i, results, firsts, lasts)
            return primal, dual, firsts, lasts

        return chunks(parts[half][1], body, (zero, zero, zero, zero), parts[half][0])

    def first_sweep(i, at, carry):
        rs = pl.ds(at, CH)
        results = []
        for r in range(rows):
            value = abun[rs, lanes(r)] * 0.2
            w1[0, rs, lanes(r)] = value
            results.append(value)
        return pack(i, results, *carry)

    def data_terms(first_time, last):
        def body(i, at, carry):
            primal, dual = carry
            rs = pl.ds(at, CH)
            for r in range(rows):
                old = d1[rs, lanes(r)]
                u = image[rs, lanes(r)] - old
                new = (spec_ref[rs, r, :] + MU * u) / (1.0 + MU)
                d_new = new - u
                res = old - d_new
                change = new - v1[rs, lanes(r)]
                primal = primal + fold(res * res)
                dual = dual + fold(change * change)
                if not last:
                    d1[rs, lanes(r)] = d_new
                    v1[rs, lanes(r)] = new
                    put_rhs(at, r, new + d_new)
            return primal, dual

        return body

    def point_terms(first_time, last):
        def body(i, at, carry):
            primal, dual = carry
            rs = pl.ds(at, CH)
            for r in range(rows):
                a = abun[rs, lanes(r)]
                old2 = None if first_time else d2[rs, lanes(r)]
                u2 = a if first_time else a - old2
                cut = jnp.clip(u2, -thresh, thresh)
                new2 = u2 - cut
                res2 = cut if first_time else old2 + cut
                change2 = new2 if first_time else new2 - v2[rs, lanes(r)]
                old5 = None if first_time else d5[rs, lanes(r)]
                u5 = a if first_time else a - old5
                new5 = jnp.maximum(u5, 0.0)
                res5 = a - new5
                change5 = new5 if first_time else new5 - v5[rs, lanes(r)]
                primal = primal + fold(res2 * res2 + res5 * res5)
                dual = dual + fold(change2 * change2 + change5 * change5)
                if last:
                    out_ref[rs, r, :] = a
                else:
                    d2[rs, lanes(r)] = -cut
                    v2[rs, lanes(r)] = new2
                    v5[rs, lanes(r)] = new5
                    d5[rs, lanes(r)] = new5 - u5
                    mixed[rs, lanes(r)] = mixed[rs, lanes(r)] + ((new2 - cut) + jnp.abs(u5))
            return primal, dual

        return body

    def second_sweep(k, half, last):
        e = 2 * k
        source = w1.at[k]
        first_time = k == 0
        pl_left = colbuf[e, half, 0]
        pl_right = colbuf[e, half, 1]

        def body(i, at, carry):
            primal, dual, firsts, lasts = carry
            rs = pl.ds(at, CH)
            x = [source[rs, lanes(r)] for r in range(rows)]
            above = rowbuf[e, 0, rs, :]
            below = rowbuf[e, 1, rs, :]
            results = []
            for r in range(rows):
                nxt = x[r + 1] if r + 1 < rows else below
                prv = x[r - 1] if r else above
                near = (prv + nxt) + (
                    from_left(i, r, x[r], pl_left) + from_right(i, r, x[r], pl_right)
                )
                a = abun[rs, lanes(r)]
                total = a if first_time else rhs[rs, lanes(r)]
                new = (total + near) * 0.2
                w3[k, rs, lanes(r)] = new
                results.append(new)
                res = a - new
                change = new if first_time else new - w3[k - 1, rs, lanes(r)]
                primal = primal + fold(res * res)
                dual = dual + fold(change * change)
                if not last:
                    d_new = new - a if first_time else new - (a - d3[rs, lanes(r)])
                    d3[rs, lanes(r)] = d_new
                    put_rhs(at, r, mixed[rs, lanes(r)] + (new + d_new))
            firsts, lasts = pack(i, results, firsts, lasts)
            return primal, dual, firsts, lasts

        return chunks(parts[half][1], body, (zero, zero, zero, zero), parts[half][0])

    tables = [None] * PARTS
    partial = [[zero, zero] for _ in range(ITERS)]

    def add(k, pair):
        partial[k][0] = partial[k][0] + pair[0]
        partial[k][1] = partial[k][1] + pair[1]

    def put_abun(i, at, carry):
        for r in range(rows):
            put_rhs(at, r, abun[pl.ds(at, CH), lanes(r)])
        return carry

    def image_terms(k, last):
        chunks(endm, put_abun, 0)
        image[...] = dot(lib3[...], rhs3[...])
        add(k, chunks(bands, data_terms(k == 0, last), (zero, zero)))

    for k in range(ITERS):
        last = k == ITERS - 1
        abun[...] = dot(inv3[...], rhs3[...])
        if k:
            image_terms(k, last)
        for half in range(PARTS):
            if k == 0:
                firsts, lasts = chunks(parts[half][1], first_sweep, (zero, zero), parts[half][0])
            else:
                primal, dual, firsts, lasts = gradients(k, half, tables[half], False)
                add(k - 1, (primal, dual))
            tables[half] = send(2 * k, half, w1.at[k], firsts, lasts)
        if k == 0:
            image_terms(k, last)
        if not last:
            mixed[...] = dot(libt3[...], rhs3[...])
        add(k, chunks(endm, point_terms(k == 0, last), (zero, zero)))
        for half in range(PARTS):
            receive(tables[half])
            primal, dual, firsts, lasts = second_sweep(k, half, last)
            add(k, (primal, dual))
            ends = (1, 3) if last else (0, 1, 2, 3)
            tables[half] = send(2 * k + 1, half, w3.at[k], firsts, lasts, ends)
    for half in range(PARTS):
        add(ITERS - 1, gradients(ITERS, half, tables[half], True)[:2])

    def gather(stage, value, index, peers, slots):
        slots[index] = value
        summing[stage] = value
        table = [
            pltpu.make_async_remote_copy(
                src_ref=summing.at[stage], dst_ref=slots.at[index],
                send_sem=sum_send.at[stage, i], recv_sem=sum_recv.at[stage, i],
                device_id=peer, device_id_type=mesh_type,
            )
            for i, peer in enumerate(peers)
        ]
        for copy in table:
            copy.start()
        pending.extend(table)
        for copy in table:
            copy.wait_recv()
        total = slots[0]
        for i in range(1, len(peers) + 1):
            total = total + slots[i]
        return total

    sums = [jnp.sum(partial[k][0], axis=0, keepdims=True) for k in range(ITERS)]
    sums += [jnp.sum(partial[k][1], axis=0, keepdims=True) * (MU * MU) for k in range(ITERS)]
    totals = gather(0, jnp.concatenate(sums, axis=0), me_r, row_peers, row_slots)
    totals = gather(1, totals, me_c, col_peers, col_slots)
    numel = float(endm * rows * cols * n_rows * n_cols)
    final = jnp.sqrt(jnp.sum(totals, axis=1, keepdims=True) / numel)
    norm_ref[:, 0:1] = final[0:ITERS]
    norm_ref[:, 1:2] = final[ITERS : 2 * ITERS]
    for copy in pending:
        copy.wait_send()


def local(spectra, library):
    bands, rows, cols = spectra.shape
    endm = library.shape[1]
    n_rows, n_cols = lax.axis_size("rows"), lax.axis_size("cols")
    pad = -(-max(bands, endm) // 256) * 256
    wide = rows * cols
    dims = (bands, endm, rows, cols, n_rows, n_cols, pad)
    field = pltpu.VMEM((endm, wide), F32)
    full = pltpu.VMEM((pad, wide), F32)
    band = pltpu.VMEM((bands, wide), F32)
    square = pltpu.VMEM((pad, pad), F32)
    stacked = pltpu.VMEM((pad, 3 * pad), BF16)
    exchanges = 2 * ITERS
    abundance, norms = pl.pallas_call(
        functools.partial(kernel, dims),
        out_shape=(
            jax.ShapeDtypeStruct((endm, rows, cols), F32),
            jax.ShapeDtypeStruct((ITERS, 2), F32),
        ),
        in_specs=[pl.BlockSpec(memory_space=pltpu.VMEM)] * 2,
        out_specs=(pl.BlockSpec(memory_space=pltpu.VMEM),) * 2,
        scratch_shapes=[
            stacked, stacked, stacked, pltpu.VMEM((3 * pad, wide), BF16),
            square, square, square,
            full, full, full, field, band, band, field, field, field, field, field,
            field, field, field, field, pltpu.VMEM((endm, cols), F32), pltpu.VMEM((PARTS, 8, cols), F32),
            pltpu.VMEM((ITERS, endm, wide), F32), pltpu.VMEM((ITERS, endm, wide), F32),
            pltpu.VMEM((exchanges, 2, endm, cols), F32),
            pltpu.VMEM((exchanges, PARTS, 2, 8, cols), F32),
            pltpu.VMEM((exchanges, PARTS, 2, 8, cols), F32),
            pltpu.SemaphoreType.DMA((exchanges, PARTS, 4)),
            pltpu.SemaphoreType.DMA((exchanges, PARTS, 4)),
            pltpu.VMEM((2, 8, cols), F32),
            pltpu.VMEM((n_rows, 8, cols), F32),
            pltpu.VMEM((n_cols, 8, cols), F32),
            pltpu.SemaphoreType.DMA((2, max(n_rows, n_cols))),
            pltpu.SemaphoreType.DMA((2, max(n_rows, n_cols))),
        ],
        compiler_params=pltpu.CompilerParams(
            collective_id=0, has_side_effects=True, vmem_limit_bytes=56 * 1024 * 1024
        ),
    )(spectra, library)
    return abundance, norms


def solution(mesh):
    placed = (P(None, "rows", "cols"), P())
    return jax.shard_map(
        local, mesh=mesh, in_specs=placed, out_specs=(P(None, "rows", "cols"), P()), check_vma=False
    )
```
